256 devices in a mesh: row: 16 (over y_lo, x, core), col: 16 (over z, y_hi).
Axes of the slice: x: 4, y: 4 (y_hi: 2, y_lo: 2; y = y_hi * 2 + y_lo), z: 8, core: 2. Of those that a mesh axis runs over, the one named last changes fastest.
Arguments:
- tokens: bfloat16 [2048, 8192], P('row', 'col'), may hold values from -200 to 200
- norm_gain: float32 [8192], P('col'), may hold values from 0.1 to 1.9
- gate_weight: bfloat16 [8192, 28672], P('col', 'row'), may hold values from -0.0625 to 0.0625
- up_weight: bfloat16 [8192, 28672], P('col', 'row'), may hold values from -0.0625 to 0.0625
- down_weight: bfloat16 [28672, 8192], P('row', 'col'), may hold values from -0.03125 to 0.03125
Outputs:
- mixed: bfloat16 [2048, 8192], P('row', 'col')
The draws below stay inside these ranges and needn't reach their ends.
All inputs are finite; a program needn't handle non-finite values.
Results may differ from the reference program's by a relative error of at most 0.028.
Values may be sent and summed in bfloat16 or wider, within the bound.
A program may use at most 128 MiB of HBM per device.

```python
import math
import jax
import jax.numpy as jnp
from jax import lax

D = 8192
FF = 28672
TOKENS = 2048
N_ROW = 16
N_COL = 16


def draw_tokens(key, part):
    first, second, third = jax.random.split(jax.random.fold_in(key, 11), 3)
    ramp = jnp.sqrt(1.0 + 2.0 * jnp.arange(D, dtype=jnp.float32) / max(D - 1, 1))
    rough = jnp.exp(jax.random.uniform(second, (D,), jnp.float32, -0.35, 0.35))
    column_scale = ramp * rough
    base = jax.random.normal(first, (TOKENS, D), jnp.float32)
    row_scale = jnp.exp(jax.random.uniform(third, (TOKENS, 1), jnp.float32, 0.0, math.log(10.0)))
    values = jnp.clip(base * column_scale[None, :] * row_scale, -200.0, 200.0)
    return values.astype(jnp.bfloat16)


def level_of(rng, extent, shards, least, largest):
    factor_of = 1.0
    for axis_at, blocks in shards:
        heights = jax.random.uniform(jax.random.fold_in(jax.random.fold_in(rng, 6), axis_at), (blocks,), jnp.float32, least / len(shards), largest / len(shards))
        factor_of = factor_of * jnp.repeat(jnp.exp(heights), extent[axis_at] // blocks).reshape((-1,) + (1,) * (len(extent) - 1 - axis_at))
    return factor_of


def gaussian(stream_key, extent, width, most, cuts=(), kind=jnp.bfloat16):
    level = level_of(stream_key, extent, cuts, -0.22, 0.18) if cuts else 1.0
    array = jax.random.normal(stream_key, extent, jnp.float32) * width * level
    return jnp.minimum(jnp.maximum(array, -most), most).astype(kind)


def setup_inputs(seed: int = 0) -> dict:
    streams_of = jax.random.split(jax.random.key(seed), 6)
    tokens = draw_tokens(jax.random.fold_in(streams_of[5], 71), 0)
    norm_gain = jnp.clip(1.0 + 0.18 * jax.random.normal(streams_of[1], (D,), jnp.float32), 0.1, 1.9)
    gate_weight = gaussian(streams_of[2], (D, FF), D ** -0.5, 0.0625, ((0, 16), (1, 16)))
    up_weight = gaussian(streams_of[3], (D, FF), D ** -0.5, 0.0625, ((0, 16), (1, 16)))
    down_weight = gaussian(streams_of[4], (FF, D), FF ** -0.5, 0.03125, ((0, 16), (1, 16)))
    return {"tokens": tokens, "norm_gain": norm_gain, "gate_weight": gate_weight, "up_weight": up_weight, "down_weight": down_weight}


def reference(tokens, norm_gain, gate_weight, up_weight, down_weight):
    values = tokens.astype(jnp.float32)
    squares = lax.optimization_barrier(jnp.sum(values * values, axis=1))
    scale = lax.rsqrt(squares / D + 1e-05)
    normed = (values * scale[:, None] * norm_gain[None, :]).astype(jnp.bfloat16)
    group = D // N_COL
    gate = jnp.zeros((TOKENS, FF), jnp.float32)
    up = jnp.zeros((TOKENS, FF), jnp.float32)
    for index in range(N_COL):
        rows = normed[:, index * group:(index + 1) * group]
        part_gate = jnp.dot(rows, gate_weight[index * group:(index + 1) * group], preferred_element_type=jnp.float32)
        part_up = jnp.dot(rows, up_weight[index * group:(index + 1) * group], preferred_element_type=jnp.float32)
        gate = gate + part_gate.astype(jnp.bfloat16).astype(jnp.float32)
        up = up + part_up.astype(jnp.bfloat16).astype(jnp.float32)
    hidden = (jax.nn.silu(gate) * up).astype(jnp.bfloat16)
    hgroup = FF // N_ROW
    mixed = jnp.zeros((TOKENS, D), jnp.float32)
    for index in range(N_ROW):
        part = jnp.dot(hidden[:, index * hgroup:(index + 1) * hgroup], down_weight[index * hgroup:(index + 1) * hgroup], preferred_element_type=jnp.float32)
        mixed = mixed + part.astype(jnp.bfloat16).astype(jnp.float32)
    return mixed.astype(jnp.bfloat16)
```

```python
import functools

import jax
import jax.numpy as jnp
from jax import lax
from jax.experimental import pallas as pl
from jax.experimental.pallas import tpu as pltpu
from jax.sharding import Mesh
from jax.sharding import PartitionSpec as P

MESH = pl.DeviceIdType.MESH
D = 8192
ROW = ("ylo", "x", "core")
COL = ("z", "yhi")
F32 = jnp.float32
BF16 = jnp.bfloat16
NZ = 8
NX = 4
NY = 4
PLANE = NX * NY
ROWS = 128
PIECE = ROWS // NZ
HALF = ROWS // 2
DS = 512
LANES = 128
NI = 7


def kernel(
    tok, gain, gate_w, up_w, down_w, out,
    X, Xg, W1, W2, R0, RS, H, O, OR, gsend, gbuf, sq, sqr, S,
    sem_g, sem_xy, sem_xx, sem_w, sem_wc, sem_w2, sem_sq, sem_rs, sem_ag, sem_o,
    snd_g, snd_xy, snd_xx, snd_xf, snd_w, snd_wc, snd_w2, snd_w2c, snd_sq, snd_rs, snd_ag, snd_agh, snd_o,
):
    ylo, x, core = (lax.axis_index(a) for a in ROW)
    z, yhi = (lax.axis_index(a) for a in COL)
    y = 2 * yhi + ylo
    mine = ylo * NX + x

    def remote(src, dst, send, recv, device):
        pltpu.make_async_remote_copy(
            src_ref=src, dst_ref=dst, send_sem=send, recv_sem=recv, device_id=device, device_id_type=MESH
        ).start()

    def arrived(ref, sem):
        pltpu.make_async_copy(ref, ref, sem).wait()

    def at_y(q):
        to = lax.rem(y + q, NY)
        return lax.rem(to, 2), to // 2

    def at_x(q):
        return lax.rem(x + q, NX)

    def at_z(q):
        return lax.rem(z + q + NZ, NZ)

    def in_plane(p):
        lo, hi = at_y(p // NX)
        return lo, hi, at_x(lax.rem(p, NX))

    barrier = pltpu.get_barrier_semaphore()

    @pl.loop(1, PLANE)
    def _(p):
        lo, hi, to_x = in_plane(p)
        pl.semaphore_signal(barrier, inc=1, device_id={"ylo": lo, "yhi": hi, "x": to_x}, device_id_type=MESH)

    @pl.loop(1, NZ)
    def _(p):
        pl.semaphore_signal(barrier, inc=1, device_id={"z": at_z(p)}, device_id_type=MESH)

    pl.semaphore_signal(barrier, inc=1, device_id={"core": 1 - core}, device_id_type=MESH)
    gsend[...] = jnp.broadcast_to(gain[...], gsend.shape)
    pl.semaphore_wait(barrier, PLANE - 1 + NZ - 1 + 1)

    def block_at(o):
        return at_z(lax.select(lax.rem(o, 2) == 1, (7 - o) // 2, 4 + o // 2))

    def own_piece(j):
        return tok.at[pl.ds(pl.multiple_of(j * PIECE, PIECE), PIECE)]

    def slot(j, row, half):
        return X.at[j, pl.ds(pl.multiple_of(row * PIECE, PIECE), PIECE), pl.ds(pl.multiple_of(half * DS, DS), DS)]

    @pl.loop(0, NZ)
    def _(o):
        j = block_at(o)
        for q in range(1, NY):
            lo, hi = at_y(q)
            remote(own_piece(j), slot(j, mine, yhi), snd_xy.at[q - 1], sem_xy.at[o], {"ylo": lo, "yhi": hi})

    for h in range(2):
        remote(gsend, gbuf.at[yhi], snd_g, sem_g, {"ylo": 1 - ylo, "yhi": h})

    half_width = NI * LANES

    @pl.loop(0, NI)
    def _(i):
        for h in range(2):
            columns = pl.ds(pl.multiple_of(h * half_width + i * LANES, LANES), LANES)
            rows = pl.ds(pl.multiple_of(yhi * DS, DS), DS)
            device = {"ylo": 1 - ylo, "yhi": h}
            remote(gate_w.at[:, columns], W1.at[i, core, rows, pl.ds(0, LANES)], snd_w, sem_w.at[i], device)
            remote(up_w.at[:, columns], W1.at[i, core, rows, pl.ds(LANES, LANES)], snd_w, sem_w.at[i], device)

    for h in range(2):
        remote(
            down_w.at[pl.ds(h * half_width, half_width)],
            W2.at[core, :, pl.ds(pl.multiple_of(yhi * DS, DS), DS)],
            snd_w2, sem_w2.at[0], {"ylo": 1 - ylo, "yhi": h},
        )

    @pl.loop(0, NZ)
    def _(o):
        j = block_at(o)
        for q in range(1, NX):
            remote(own_piece(j), slot(j, mine, yhi), snd_xx.at[q - 1], sem_xx.at[o], {"x": at_x(q)})
        X[j, pl.ds(pl.multiple_of(mine * PIECE, PIECE), PIECE), pl.ds(pl.multiple_of(yhi * DS, DS), DS)] = tok[
            pl.ds(pl.multiple_of(j * PIECE, PIECE), PIECE)
        ]
        arrived(X.at[0, pl.ds(0, 3 * PIECE), pl.ds(0, DS)], sem_xy.at[o])
        for r in range(1, NY):
            lo, hi = at_y(r)
            for q in range(1, NX):
                ref = slot(j, lo * NX + x, hi)
                remote(ref, ref, snd_xf.at[r - 1, q - 1], sem_xx.at[o], {"x": at_x(q)})

    arrived(gbuf, sem_g)

    def prepare(o):
        j = block_at(o)
        arrived(X.at[0, pl.ds(0, 6 * PIECE)], sem_xx.at[o])
        values = X[j].astype(F32)
        parts = [values[:, k * LANES : (k + 1) * LANES] for k in range(2 * DS // LANES)]
        total = functools.reduce(jnp.add, [part * part for part in parts])
        sq[j] = jnp.broadcast_to(jnp.sum(total.T, axis=0, keepdims=True), (8, LANES))
        for h in range(2):
            Xg[j, :, h * DS : (h + 1) * DS] = (values[:, h * DS : (h + 1) * DS] * gbuf[h, 0:1, :]).astype(BF16)
        return j

    def prepare_and_send(o):
        j = prepare(o)
        p = lax.rem(j - z + NZ, NZ)
        remote(sq.at[j], sqr.at[p], snd_sq, sem_sq, {"z": j})

    def product(j, i, k):
        return jnp.dot(Xg[j], W1[i, k], preferred_element_type=F32)

    signs = (1, -1)
    halves = (pl.ds(0, HALF), pl.ds(HALF, HALF))

    def columns_of(i, k):
        return pl.ds(pl.multiple_of((k * NI + i) * LANES, LANES), LANES)

    def finish(i, k):
        for d in range(2):
            arrived(RS.at[d, 3, i, k], sem_rs.at[d, 3, i, k])
        sums = product(z, i, k) + RS[0, 3, i, k].astype(F32) + RS[1, 3, i, k].astype(F32)
        gate = sums[:, :LANES] * S[...]
        up = sums[:, LANES:] * S[...]
        columns = columns_of(i, k)
        H[z, :, columns] = (gate / (1.0 + jnp.exp(-gate)) * up).astype(BF16)
        ref = H.at[z, :, columns]
        for d in range(2):
            remote(ref, ref, snd_ag.at[d, 0], sem_ag.at[d, 0, i, k], {"z": at_z(signs[d])})

    def pass_on(s, i, k):
        for d in range(2):
            j = at_z(signs[d] * (4 - s))
            ref = RS.at[d, s - 1, i, k]
            p = product(j, i, k)
            if s == 1:
                arrived(ref.at[halves[d]], sem_rs.at[d, 0, i, k])
                other = halves[1 - d]
                a, b = d * HALF, (1 - d) * HALF
                RS[d, 0, i, k, halves[d]] = (p[a : a + HALF] + RS[d, 0, i, k, halves[d]].astype(F32)).astype(BF16)
                RS[d, 0, i, k, other] = p[b : b + HALF].astype(BF16)
            else:
                arrived(ref, sem_rs.at[d, s - 1, i, k])
                RS[d, s - 1, i, k] = (p + RS[d, s - 1, i, k].astype(F32)).astype(BF16)
            remote(ref, RS.at[d, s, i, k], snd_rs.at[d, s], sem_rs.at[d, s, i, k], {"z": at_z(signs[d])})

    def open_up(i, k):
        R0[i, k] = product(at_z(4), i, k).astype(BF16)
        for d in range(2):
            remote(
                R0.at[i, k, halves[d]], RS.at[d, 0, i, k, halves[d]],
                snd_rs.at[d, 0], sem_rs.at[d, 0, i, k], {"z": at_z(signs[d])},
            )

    def pair_of_cores(c):
        return lax.rem(core + c, 2)

    @pl.loop(0, NI + 4)
    def _(w):
        @pl.when(w == 0)
        def _():
            prepare_and_send(0)

        @pl.when((w >= 1) & (w <= 3))
        def _():
            @pl.loop(0, 2)
            def _(c):
                prepare_and_send(2 * w - 1 + c)

        @pl.when(w == 4)
        def _():
            prepare(7)
            arrived(sqr.at[pl.ds(1, NZ - 1)], sem_sq)
            total = sq[z] + functools.reduce(jnp.add, [sqr[p] for p in range(1, NZ)])
            scale = lax.rsqrt(total[0:1] / D + 1e-05)
            S[...] = jnp.broadcast_to(scale, (LANES, LANES)).T

        @pl.when(w >= 4)
        def _():
            @pl.loop(0, 2)
            def _(c):
                finish(w - 4, pair_of_cores(c))

        for s in (3, 2, 1):
            @pl.when((w >= s) & (w - s < NI))
            def _(s=s):
                @pl.loop(0, 2)
                def _(c):
                    pass_on(s, w - s, pair_of_cores(c))

        @pl.when(w < NI)
        def _():
            arrived(W1.at[w, core], sem_w.at[w])
            remote(W1.at[w, core], W1.at[w, core], snd_wc, sem_wc.at[w], {"core": 1 - core})
            open_up(w, core)
            arrived(W1.at[w, 1 - core], sem_wc.at[w])
            open_up(w, 1 - core)

    arrived(W2.at[core], sem_w2.at[0])
    remote(W2.at[core], W2.at[core], snd_w2c, sem_w2.at[1], {"core": 1 - core})

    def mix(j):
        total = jnp.dot(H[j, :, :half_width], W2[0], preferred_element_type=F32)
        total = total + jnp.dot(H[j, :, half_width:], W2[1], preferred_element_type=F32)
        O[j] = total.astype(BF16)

        @pl.loop(1, PLANE)
        def _(p):
            lo, hi, to_x = in_plane(p)
            row = pl.ds(pl.multiple_of((lo * NX + to_x) * PIECE, PIECE), PIECE)
            column = pl.ds(pl.multiple_of(hi * DS, DS), DS)
            remote(O.at[j, row, column], OR.at[j, p], snd_o, sem_o.at[j], {"ylo": lo, "yhi": hi, "x": to_x})

    def forward(a, i, k):
        columns = columns_of(i, k)
        for d in range(2):
            j = at_z(-signs[d] * a)
            whole = H.at[j, :, columns]
            arrived(whole, sem_ag.at[d, a - 1, i, k])
            if a < 3:
                remote(whole, whole, snd_ag.at[d, a], sem_ag.at[d, a, i, k], {"z": at_z(signs[d])})
            else:
                part = H.at[j, halves[d], columns]
                remote(part, part, snd_agh.at[d], sem_ag.at[d, a, i, k], {"z": at_z(signs[d])})

    for a in range(1, 4):
        @pl.loop(0, 2)
        def _(h, a=a):
            k = pair_of_cores(h)

            if a == 1:
                @pl.loop(0, NI)
                def _(i):
                    forward(a, i, k)

                @pl.when(h == 0)
                def _():
                    arrived(W2.at[1 - core], sem_w2.at[1])
                    mix(z)
            else:
                mix(at_z((1 - 2 * h) * (a - 1)))

                @pl.loop(0, NI)
                def _(i):
                    forward(a, i, k)

    @pl.loop(0, 2)
    def _(h):
        mix(at_z((1 - 2 * h) * 3))

    far = at_z(4)

    @pl.loop(0, NI)
    def _(i):
        for k in range(2):
            for d in range(2):
                arrived(H.at[far, halves[d], columns_of(i, k)], sem_ag.at[d, 3, i, k])

    mix(far)

    @pl.loop(0, NZ)
    def _(o):
        j = block_at(7 - o)
        arrived(OR.at[j, pl.ds(1, PLANE - 1)], sem_o.at[j])
        own = O[j, pl.ds(pl.multiple_of(mine * PIECE, PIECE), PIECE), pl.ds(pl.multiple_of(yhi * DS, DS), DS)]
        total = own.astype(F32) + functools.reduce(jnp.add, [OR[j, p].astype(F32) for p in range(1, PLANE)])
        out[pl.ds(pl.multiple_of(j * PIECE, PIECE), PIECE)] = total.astype(BF16)

    arrived(gbuf, snd_g)
    for q in range(3):
        arrived(tok, snd_xy.at[q])
        arrived(tok, snd_xx.at[q])
        for r in range(3):
            arrived(tok, snd_xf.at[r, q])
    arrived(W1.at[:, 0], snd_w)
    arrived(W1.at[:, 0], snd_wc)
    arrived(W2.at[0], snd_w2)
    arrived(W2.at[0], snd_w2c)
    arrived(sqr.at[pl.ds(1, NZ - 1)], snd_sq)
    for d in range(2):
        arrived(R0.at[:, :, halves[d]], snd_rs.at[d, 0])
        for s in range(1, 4):
            arrived(RS.at[d, s], snd_rs.at[d, s])
        for a in range(3):
            arrived(H.at[0], snd_ag.at[d, a])
        arrived(H.at[0, halves[d]], snd_agh.at[d])
    arrived(OR.at[:, pl.ds(1, PLANE - 1)], snd_o)


def body(tokens, norm_gain, gate_weight, up_weight, down_weight):
    vmem = pl.BlockSpec(memory_space=pltpu.VMEM)
    hbm = pl.BlockSpec(memory_space=pl.ANY)
    dma = pltpu.SemaphoreType.DMA
    return pl.pallas_call(
        kernel,
        name="swiglu",
        out_shape=jax.ShapeDtypeStruct(tokens.shape, tokens.dtype),
        in_specs=[vmem, vmem, hbm, hbm, hbm],
        out_specs=vmem,
        scratch_shapes=[
            pltpu.VMEM((NZ, ROWS, 2 * DS), BF16),
            pltpu.VMEM((NZ, ROWS, 2 * DS), BF16),
            pltpu.VMEM((NI, 2, 2 * DS, 2 * LANES), BF16),
            pltpu.VMEM((2, NI * LANES, 2 * DS), BF16),
            pltpu.VMEM((NI, 2, ROWS, 2 * LANES), BF16),
            pltpu.VMEM((2, 4, NI, 2, ROWS, 2 * LANES), BF16),
            pltpu.VMEM((NZ, ROWS, 2 * NI * LANES), BF16),
            pltpu.VMEM((NZ, ROWS, 2 * DS), BF16),
            pltpu.VMEM((NZ, PLANE, PIECE, DS), BF16),
            pltpu.VMEM((8, DS), F32),
            pltpu.VMEM((2, 8, DS), F32),
            pltpu.VMEM((NZ, 8, LANES), F32),
            pltpu.VMEM((NZ, 8, LANES), F32),
            pltpu.VMEM((LANES, LANES), F32),
            dma, dma((NZ,)), dma((NZ,)), dma((NI,)), dma((NI,)), dma((2,)), dma,
            dma((2, 4, NI, 2)), dma((2, 4, NI, 2)), dma((NZ,)),
            dma, dma((3,)), dma((3,)), dma((3, 3)), dma, dma, dma, dma, dma,
            dma((2, 4)), dma((2, 3)), dma((2,)), dma,
        ],
        compiler_params=pltpu.CompilerParams(
            collective_id=0, has_side_effects=True, vmem_limit_bytes=60 * 1024 * 1024
        ),
    )(tokens, norm_gain.reshape(1, -1), gate_weight, up_weight, down_weight)


def solution(mesh):
    torus = Mesh(mesh.devices.reshape(2, NX, 2, NZ, 2), ROW + COL)
    return jax.shard_map(
        body,
        mesh=torus,
        in_specs=(P(ROW, COL), P(COL), P(COL, ROW), P(COL, ROW), P(ROW, COL)),
        out_specs=P(ROW, COL),
        check_vma=False,
    )
```

```python
import functools

import jax
import jax.numpy as jnp
from jax import lax
from jax.experimental import pallas as pl
from jax.experimental.pallas import tpu as pltpu
from jax.sharding import Mesh
from jax.sharding import PartitionSpec as P

MESH = pl.DeviceIdType.MESH
D = 8192
ROW = ("ylo", "x", "core")
COL = ("z", "yhi")
F32 = jnp.float32
BF16 = jnp.bfloat16
NZ = 8
NX = 4
NY = 4
PLANE = NX * NY
ROWS = 128
PIECE = ROWS // NZ
HALF = ROWS // 2
DS = 512
LANES = 128
NI = 7
LAG = (0, 1, 2, 3, 6)
Y = (3, 5, 6)
A = (3, 5, 5)
CUT = 4
RING = 3
FILL = 1
EARLY = 4


def kernel(
    tok, gain, gate_w, up_w, down_w, out,
    T, X, Xg, W1, W2, R0, RS, H, O, OR, gown, gbuf, sq, sqr, S, known,
    sem_t, sem_g, sem_xy, sem_xx, sem_w, sem_wc, sem_w2, sem_sq, sem_rs, sem_r2, sem_r3, sem_ag, sem_ah, sem_o,
    snd_g, snd_x, snd_w, snd_w2, snd_sq, snd_rs, snd_h, snd_o,
):
    ylo, x, core = (lax.axis_index(a) for a in ROW)
    z, yhi = (lax.axis_index(a) for a in COL)
    y = 2 * yhi + ylo

    def remote(src, dst, send, recv, device):
        pltpu.make_async_remote_copy(
            src_ref=src, dst_ref=dst, send_sem=send, recv_sem=recv, device_id=device, device_id_type=MESH
        ).start()

    def arrived(ref, sem):
        pltpu.make_async_copy(ref, ref, sem).wait()

    def at_y(q):
        to = lax.rem(y + q, NY)
        return lax.rem(to, 2), to // 2

    def at_x(q):
        return lax.rem(x + q + NX, NX)

    def at_z(q):
        return lax.rem(z + q + NZ, NZ)

    def in_plane(p):
        lo, hi = at_y(p // NX)
        return lo, hi, at_x(lax.rem(p, NX))

    def tile(at, size):
        return pl.ds(pl.multiple_of(at * size, size), size)

    loads = [pltpu.make_async_copy(tok, T, sem_t.at[0]), pltpu.make_async_copy(gain, gown, sem_t.at[1])]
    for load in loads:
        load.start()

    barrier = pltpu.get_barrier_semaphore()

    @pl.loop(1, NZ)
    def _(p):
        pl.semaphore_signal(barrier, inc=1, device_id={"z": at_z(p)}, device_id_type=MESH)

    @pl.loop(1, PLANE)
    def _(p):
        lo, hi, to_x = in_plane(p)
        pl.semaphore_signal(barrier, inc=1, device_id={"ylo": lo, "yhi": hi, "x": to_x}, device_id_type=MESH)

    pl.semaphore_signal(barrier, inc=1, device_id={"core": 1 - core}, device_id_type=MESH)
    for load in loads:
        load.wait()

    @pl.loop(0, NZ)
    def _(j):
        X[j, tile(x * 2 + ylo, PIECE), tile(yhi, DS)] = T[tile(j, PIECE)]

    pl.semaphore_wait(barrier, PLANE - 1 + NZ - 1 + 1)

    def block_at(o):
        return at_z(lax.select(lax.rem(o, 2) == 1, (7 - o) // 2, 4 + o // 2))

    def along_y(o):
        j = block_at(o)
        for q in (2, 1, 3):
            lo, hi = at_y(q)
            remote(
                T.at[tile(j, PIECE)], X.at[j, tile(x * 2 + ylo, PIECE), tile(yhi, DS)],
                snd_x, sem_xy.at[o], {"ylo": lo, "yhi": hi},
            )

    def weights(i):
        for h in range(2):
            columns = tile(h * NI + i, LANES)
            device = {"ylo": 1 - ylo, "yhi": h}
            remote(gate_w.at[:, columns], W1.at[i, core, tile(yhi, DS), pl.ds(0, LANES)], snd_w, sem_w.at[i], device)
            remote(up_w.at[:, columns], W1.at[i, core, tile(yhi, DS), pl.ds(LANES, LANES)], snd_w, sem_w.at[i], device)

    for i, (first, end) in enumerate(((0, Y[0]), (Y[0], Y[1]), (Y[1], Y[2]))):
        @pl.loop(first, end)
        def _(o):
            along_y(o)

        if i == 0:
            for h in range(2):
                remote(gown, gbuf.at[yhi], snd_g, sem_g, {"ylo": 1 - ylo, "yhi": h})

        weights(i)

    @pl.loop(Y[2], NZ)
    def _(o):
        along_y(o)

    @pl.loop(3, NI)
    def _(i):
        weights(i)

    @pl.loop(0, NI)
    def _(i):
        for h in range(2):
            remote(
                down_w.at[tile(h * NI + i, LANES)], W2.at[i, core, :, tile(yhi, DS)],
                snd_w2, sem_w2.at[0], {"ylo": 1 - ylo, "yhi": h},
            )

    def own_along_x(o):
        ref = X.at[block_at(o), tile(x * 2 + ylo, PIECE), tile(yhi, DS)]
        for q in (2, 1, 3):
            remote(ref, ref, snd_x, sem_xx.at[o], {"x": at_x(q)})

    def along_x(o):
        j = block_at(o)
        arrived(X.at[0, pl.ds(0, 3 * PIECE), pl.ds(0, DS)], sem_xy.at[o])
        for ref in (
            X.at[j, tile(x * 2 + 1 - ylo, PIECE)],
            X.at[j, tile(x * 2 + ylo, PIECE), tile(1 - yhi, DS)],
        ):
            for q in (2, 1, 3):
                remote(ref, ref, snd_x, sem_xx.at[o], {"x": at_x(q)})

    def prepare(o):
        j = block_at(o)
        arrived(X.at[0, pl.ds(0, 6 * PIECE)], sem_xx.at[o])
        values = X[j].astype(F32)
        parts = [values[:, k * LANES : (k + 1) * LANES] for k in range(2 * DS // LANES)]
        total = functools.reduce(jnp.add, [part * part for part in parts])
        sq[j] = jnp.broadcast_to(jnp.sum(total.T, axis=0, keepdims=True), (8, LANES))
        for h in range(2):
            Xg[j, :, h * DS : (h + 1) * DS] = (values[:, h * DS : (h + 1) * DS] * gbuf[h, 0:1, :]).astype(BF16)
        return j

    def prepare_and_send(o):
        j = prepare(o)
        p = lax.rem(j - z + NZ, NZ)
        remote(sq.at[j], sqr.at[p], snd_sq, sem_sq, {"z": j})

    signs = (1, -1)
    halves = (pl.ds(0, HALF), pl.ds(HALF, HALF))

    def pair(i):
        return tile(i, 2 * LANES)

    def finish(i):
        arrived(RS.at[:, 3, i], sem_r3.at[i])

        @pl.loop(0, 2)
        def _(k):
            p = jnp.dot(Xg[z], W1[i, k], preferred_element_type=F32)
            sums = p + RS[0, 3, i, k].astype(F32) + RS[1, 3, i, k].astype(F32)
            gate = sums[:, :LANES] * S[...]
            up = sums[:, LANES:] * S[...]
            H[z, :, tile(2 * i + k, LANES)] = (gate / (1.0 + jnp.exp(-gate)) * up).astype(BF16)

    def spread(i):
        ref = H.at[z, :, pair(i)]
        for d in range(2):
            remote(ref, ref, snd_h, sem_ag.at[0, i // 2], {"z": at_z(signs[d])})

    def ring(s, i, k):
        if s < 2:
            return sem_rs.at[s, lax.rem(i, RING), k]
        return sem_r2.at[lax.rem(i, RING + 1)] if s == 2 else sem_r3.at[i]

    def pass_on(s, i, k, both_cores):
        blocks = [at_z(signs[d] * (4 - s)) for d in range(2)]
        both = jnp.dot(
            jnp.concatenate([Xg[blocks[0]], Xg[blocks[1]]], axis=0), W1[i, k], preferred_element_type=F32
        )
        if s < 3:
            arrived(RS.at[0, 0, i, k] if s == 1 else RS.at[:, 1, i, k], ring(s - 1, i, k))
        elif both_cores:
            arrived(RS.at[:, 2, i], ring(2, i, k))
        for d in range(2):
            ref = RS.at[d, s - 1, i, k]
            p = both[d * ROWS : (d + 1) * ROWS]
            if s == 1:
                a, b = d * HALF, (1 - d) * HALF
                RS[d, 0, i, k, halves[d]] = (p[a : a + HALF] + RS[d, 0, i, k, halves[d]].astype(F32)).astype(BF16)
                RS[d, 0, i, k, halves[1 - d]] = p[b : b + HALF].astype(BF16)
            else:
                RS[d, s - 1, i, k] = (p + RS[d, s - 1, i, k].astype(F32)).astype(BF16)
            remote(ref, RS.at[d, s, i, k], snd_rs, ring(s, i, k), {"z": at_z(signs[d])})

    def open_up(i, k):
        R0[i, k] = jnp.dot(Xg[at_z(4)], W1[i, k], preferred_element_type=F32).astype(BF16)
        for d in range(2):
            remote(
                R0.at[i, k, halves[d]], RS.at[d, 0, i, k, halves[d]],
                snd_rs, ring(0, i, k), {"z": at_z(signs[d])},
            )

    def group(g):
        return pl.ds(g * 4 * LANES, min(4 * LANES, 2 * NI * LANES - g * 4 * LANES))

    def forward(g):
        arrived(H.at[pl.ds(0, 2), :, group(g)], sem_ag.at[0, g])
        for d in range(2):
            ref = H.at[at_z(-signs[d]), :, group(g)]
            remote(ref, ref, snd_h, sem_ag.at[1, g], {"z": at_z(signs[d])})

    @pl.loop(0, EARLY)
    def _(o):
        own_along_x(o)

    @pl.loop(0, A[0])
    def _(o):
        along_x(o)

    arrived(gbuf, sem_g)
    last = NI + LAG[4] - 1

    @pl.loop(0, last + 1)
    def _(w):
        def stage(s):
            return (w >= LAG[s]) & (w < NI + LAG[s])

        def later(s, k, both_cores):
            @pl.when(stage(s))
            def _():
                pass_on(s, w - LAG[s], k, both_cores)

        def prepare_for(s):
            @pl.when(w == LAG[s])
            def _():
                @pl.loop(max(2 * s - 1, 0), 2 * s + 1)
                def _(o):
                    prepare_and_send(o)

        @pl.when(w == last)
        def _():
            for g in range(FILL):
                forward(g)

        prepare_for(2)
        later(2, core, False)
        prepare_for(1)
        later(1, core, False)
        later(2, 1 - core, False)
        prepare_for(0)

        @pl.when(stage(0))
        def _():
            arrived(W1.at[w, core], sem_w.at[w])
            remote(W1.at[w, core], W1.at[w, core], snd_w, sem_wc.at[lax.rem(w, 2)], {"core": 1 - core})
            open_up(w, core)

        later(1, 1 - core, False)

        @pl.when(w == LAG[4])
        def _():
            prepare(7)
            arrived(sqr.at[pl.ds(1, NZ - 1)], sem_sq)
            total = sq[z] + functools.reduce(jnp.add, [sqr[p] for p in range(1, NZ)])
            scale = lax.rsqrt(total[0:1] / D + 1e-05)
            S[...] = jnp.broadcast_to(scale, (LANES, LANES)).T

        @pl.when(stage(4))
        def _():
            finish(w - LAG[4])
            spread(w - LAG[4])

        prepare_for(3)
        later(3, 1 - core, True)

        @pl.when(w == 0)
        def _():
            @pl.loop(A[0], A[1])
            def _(o):
                along_x(o)

        @pl.when(w == 1)
        def _():
            @pl.loop(EARLY, NZ)
            def _(o):
                own_along_x(o)

            @pl.loop(A[1], A[2])
            def _(o):
                along_x(o)

        @pl.when(w == 2)
        def _():
            @pl.loop(A[2], NZ)
            def _(o):
                along_x(o)

        later(3, core, False)

        @pl.when(stage(0))
        def _():
            arrived(W1.at[w, 1 - core], sem_wc.at[lax.rem(w, 2)])
            open_up(w, 1 - core)

        @pl.when(w == NI + 1)
        def _():
            arrived(W2.at[:, core], sem_w2.at[0])
            remote(W2.at[:, core], W2.at[:, core], snd_w2, sem_w2.at[1], {"core": 1 - core})

    def mixed(rows):
        return jnp.dot(rows, W2[...].reshape(2 * NI * LANES, 2 * DS), preferred_element_type=F32).astype(BF16)

    def landed(u):
        return sem_o.at[max(u - 4, 0) if isinstance(u, int) else 0]

    def deliver(u, p, lo, hi, to_x):
        remote(
            O.at[u, tile(to_x * 2 + lo, PIECE), tile(hi, DS)], OR.at[u, p],
            snd_o, landed(u), {"ylo": lo, "yhi": hi, "x": to_x},
        )

    def mix(u, top, bottom=None):
        O[u] = mixed(
            H[top] if bottom is None else jnp.concatenate([H[top, :HALF], H[bottom, HALF:]], axis=0)
        )

        @pl.loop(1, PLANE)
        def _(p):
            deliver(u, p, *in_plane(p))

    def mix_quarters(u, top, bottom, h, known=None, first=0):
        a, b = h * HALF // 2, HALF + h * HALF // 2
        columns = slice(2 * LANES * first, None)
        rows = jnp.concatenate(
            [H[top, a : a + HALF // 2, columns], H[bottom, b : b + HALF // 2, columns]], axis=0
        )
        for n in (1, 0):
            hi = lax.rem(yhi + n, 2)
            weight = W2[first:, :, :, tile(hi, DS)].reshape((NI - first) * 2 * LANES, DS)
            total = jnp.dot(rows, weight, preferred_element_type=F32)
            if known is not None:
                total = total + known[:, tile(hi, DS)]
            total = total.astype(BF16)
            O[u, a : a + HALF // 2, tile(hi, DS)] = total[: HALF // 2]
            O[u, b : b + HALF // 2, tile(hi, DS)] = total[HALF // 2 :]
            for c in (n + 1, n):
                for e in (1, 0):
                    lo = lax.rem(ylo + c, 2)
                    to_x = h + 2 * lax.rem(x // 2 + e, 2)
                    p = lax.rem(2 * hi + lo - y + NY, NY) * NX + lax.rem(to_x - x + NX, NX)

                    @pl.when(p != 0)
                    def _(p=p, lo=lo, hi=hi, to_x=to_x):
                        deliver(u, p, lo, hi, to_x)

    def half(d, a, h, columns):
        return H.at[at_z(-signs[d] * a), halves[h], columns]

    groups = range(4)
    for g in groups[FILL:]:
        forward(g)

    arrived(W2.at[:, 1 - core], sem_w2.at[1])
    mix(0, z)

    @pl.loop(0, 2)
    def _(h):
        mix(1 + h, at_z(1 - 2 * h))

    for g in groups:
        arrived(H.at[pl.ds(0, 2), :, group(g)], sem_ag.at[1, g])
        for d in range(2):
            ref = half(d, 2, d, group(g))
            remote(ref, ref, snd_h, sem_ag.at[2, g], {"z": at_z(signs[d])})

    for g in groups:
        arrived(H.at[0, :, group(g)], sem_ag.at[2, g])
        for d in range(2):
            ref = half(d, 3, d, group(g))
            remote(ref, ref, snd_h, sem_ah.at[0], {"z": at_z(signs[d])})
        if g < 2:
            mix(3 + g, at_z(2 - 4 * g))

    def quarter(d, a, h, columns=pl.ds(0, 2 * NI * LANES)):
        return H.at[at_z(-signs[d] * a), pl.ds((1 - d) * HALF + h * HALF // 2, HALF // 2), columns]

    cut = 2 * LANES * CUT
    parts = ((0, pl.ds(0, 2 * NI * LANES)), (1, pl.ds(0, cut)), (1, pl.ds(cut, 2 * NI * LANES - cut)))
    for n, (h, columns) in enumerate(parts):
        for d in range(2):
            ref = quarter(d, 2, h, columns)
            remote(ref, ref, snd_h, sem_ah.at[1 + n], {"z": at_z(signs[d])})

    mix(5, at_z(-3), at_z(3))

    arrived(H.at[0], sem_ah.at[0])

    mix(6, at_z(4))

    def last_arrived(n):
        arrived(H.at[0, halves[0], parts[n][1]], sem_ah.at[1 + n])

    top, bottom = at_z(3), at_z(-3)
    last_arrived(0)
    mix_quarters(7, top, bottom, 0)
    last_arrived(1)
    a, b = HALF // 2, HALF + HALF // 2
    rows = jnp.concatenate([H[top, a : a + HALF // 2, :cut], H[bottom, b : b + HALF // 2, :cut]], axis=0)
    known[...] = jnp.dot(rows, W2[:CUT].reshape(cut, 2 * DS), preferred_element_type=F32)
    last_arrived(2)
    mix_quarters(7, top, bottom, 1, known, CUT)

    def gather(u, j):
        total = functools.reduce(jnp.add, [OR[u, p].astype(F32) for p in range(1, PLANE)])
        total = total + O[u, tile(x * 2 + ylo, PIECE), tile(yhi, DS)].astype(F32)
        out[tile(j, PIECE)] = total.astype(BF16)

    arrived(OR.at[pl.ds(0, 5), pl.ds(1, PLANE - 1)], sem_o.at[0])

    @pl.loop(0, 5)
    def _(u):
        gather(u, at_z(lax.select(lax.rem(u, 2) == 1, (u + 1) // 2, -(u // 2))))

    side = lax.select(x < 2, -3, 3)
    for u, j in ((5, at_z(side)), (6, at_z(4)), (7, at_z(-side))):
        arrived(OR.at[u, pl.ds(1, PLANE - 1)], sem_o.at[u - 4])
        gather(u, j)

    arrived(gbuf, snd_g)
    arrived(X.at[:, pl.ds(0, 15 * HALF // 8)], snd_x)
    arrived(W1, snd_w)
    arrived(W2, snd_w2)
    arrived(sqr.at[pl.ds(1, NZ - 1)], snd_sq)
    arrived(RS.at[:, :, :, :, pl.ds(0, 7 * ROWS // 8)], snd_rs)
    arrived(H.at[pl.ds(0, 7)], snd_h)
    arrived(OR.at[:, pl.ds(1, PLANE - 1)], snd_o)


def body(tokens, norm_gain, gate_weight, up_weight, down_weight):
    vmem = pl.BlockSpec(memory_space=pltpu.VMEM)
    hbm = pl.BlockSpec(memory_space=pl.ANY)
    dma = pltpu.SemaphoreType.DMA
    return pl.pallas_call(
        kernel,
        name="swiglu",
        out_shape=jax.ShapeDtypeStruct(tokens.shape, tokens.dtype),
        in_specs=[hbm] * 5,
        out_specs=vmem,
        scratch_shapes=[
            pltpu.VMEM((ROWS, DS), BF16),
            pltpu.VMEM((NZ, ROWS, 2 * DS), BF16),
            pltpu.VMEM((NZ, ROWS, 2 * DS), BF16),
            pltpu.VMEM((NI, 2, 2 * DS, 2 * LANES), BF16),
            pltpu.VMEM((NI, 2, LANES, 2 * DS), BF16),
            pltpu.VMEM((NI, 2, ROWS, 2 * LANES), BF16),
            pltpu.VMEM((2, 4, NI, 2, ROWS, 2 * LANES), BF16),
            pltpu.VMEM((NZ, ROWS, 2 * NI * LANES), BF16),
            pltpu.VMEM((NZ, ROWS, 2 * DS), BF16),
            pltpu.VMEM((NZ, PLANE, PIECE, DS), BF16),
            pltpu.VMEM((1, DS), F32),
            pltpu.VMEM((2, 1, DS), F32),
            pltpu.VMEM((NZ, 8, LANES), F32),
            pltpu.VMEM((NZ, 8, LANES), F32),
            pltpu.VMEM((LANES, LANES), F32),
            pltpu.VMEM((HALF, 2 * DS), F32),
            dma((2,)), dma, dma((NZ,)), dma((NZ,)), dma((NI,)), dma((2,)), dma((2,)), dma,
            dma((2, RING, 2)), dma((RING + 1,)), dma((NI,)), dma((3, 4)), dma((4,)), dma((4,)),
            dma, dma, dma, dma, dma, dma, dma, dma,
        ],
        compiler_params=pltpu.CompilerParams(
            collective_id=0, has_side_effects=True, vmem_limit_bytes=46 * 1024 * 1024
        ),
    )(*[pltpu.with_memory_space_constraint(q, pltpu.HBM) for q in (tokens, norm_gain.reshape(1, -1), gate_weight, up_weight, down_weight)])


def solution(mesh):
    torus = Mesh(mesh.devices.reshape(2, NX, 2, NZ, 2), ROW + COL)
    return jax.shard_map(
        body,
        mesh=torus,
        in_specs=(P(ROW, COL), P(COL), P(COL, ROW), P(COL, ROW), P(ROW, COL)),
        out_specs=P(ROW, COL),
        check_vma=False,
    )
```
